32 devices in a mesh: coarse: 4 (over y, x), fine: 4 (over z), group: 2 (over core).
Axes of the slice: x: 2, y: 2, z: 4, core: 2. Of those that a mesh axis runs over, the one named last changes fastest.
Arguments:
- fresh_keys: bfloat16 [16, 8192, 8, 128], P(None, ('coarse', 'fine'), 'group'), may hold values from -6 to 6
- fresh_values: bfloat16 [16, 8192, 8, 128], P(None, ('coarse', 'fine'), 'group'), may hold values from -6 to 6
- turn_angle: float32 [8192, 64], replicated, may hold values from -3.140625 to 3.140625
- key_gain: float32 [128], replicated, may hold values from 0.25 to 1.75
Outputs:
- decode_keys: bfloat16 [16, 8, 128, 8192], P(('coarse', 'fine'), 'group')
- decode_values: bfloat16 [16, 8192, 8, 128], P(('coarse', 'fine'), None, 'group')
- key_scale: float32 [16, 8, 128], P(('coarse', 'fine'), 'group')
The draws below stay inside these ranges and needn't reach their ends.
All inputs are finite; a program needn't handle non-finite values. Where the reference program divides by a largest or mean magnitude, that divisor is 1e-20 or more.
Results may differ from the reference program's by a relative error of at most 0.001.
Values may be sent and summed in bfloat16 or wider, within the bound.
A program may use at most 128 MiB of HBM per device.

```python
import jax
import jax.numpy as jnp
from jax import lax

BATCH = 16
LENGTH = 8192
KV_HEADS = 8
HEAD_SIZE = 128
HALF_HEAD = 64


def steps_of(key, dims, pieces, least, largest):
    loudness, own = 1.0, jax.random.fold_in(key, 6)
    for dim, shards_of in pieces:
        draws = jnp.exp(jax.random.uniform(jax.random.fold_in(own, dim), (shards_of,), jnp.float32, least / len(pieces), largest / len(pieces)))
        loudness = loudness * jnp.repeat(draws, dims[dim] // shards_of).reshape([-1 if axis == dim else 1 for axis in range(len(dims))])
    return loudness


def noise(stream_key, extent, scale, limit, shards=(), held_as=jnp.bfloat16):
    factor_of = steps_of(stream_key, extent, shards, -0.22, 0.18) if shards else 1.0
    values = jax.random.normal(stream_key, extent, jnp.float32) * scale * factor_of
    return jnp.minimum(jnp.maximum(values, -limit), limit).astype(held_as)


def setup_inputs(seed: int = 0) -> dict:
    streams_of = jax.random.split(jax.random.key(seed), 5)
    return {
        "fresh_keys": noise(streams_of[0], (BATCH, LENGTH, KV_HEADS, HEAD_SIZE), 1.0, 6.0, ((1, 16), (2, 2))),
        "fresh_values": noise(streams_of[1], (BATCH, LENGTH, KV_HEADS, HEAD_SIZE), 1.0, 6.0, ((1, 16), (2, 2))),
        "turn_angle": jnp.clip(jax.random.uniform(streams_of[2], (LENGTH, HALF_HEAD), jnp.float32, -3.140625, 3.140625), -3.140625, 3.140625),
        "key_gain": jnp.clip(1.0 + 0.15 * jax.random.normal(streams_of[3], (HEAD_SIZE,), jnp.float32), 0.25, 1.75),
    }


def turn_pairs(vectors, angle):
    half = vectors.shape[-1] // 2
    cosine, sine = (jnp.cos(angle)[None, :, None, :], jnp.sin(angle)[None, :, None, :])
    first, second = (vectors[..., :half], vectors[..., half:])
    return jnp.concatenate([first * cosine - second * sine, second * cosine + first * sine], axis=-1)

def root_norm(vectors, row_gain):
    return vectors * lax.rsqrt(lax.optimization_barrier(jnp.mean(vectors * vectors, axis=-1, keepdims=True)) + 1e-06) * row_gain

def ready_to_store(plain_keys, angle, key_gain):
    wide_keys = plain_keys.astype(jnp.float32)
    wide_keys = root_norm(wide_keys, key_gain)
    return turn_pairs(wide_keys, angle)

def reference(fresh_keys, fresh_values, turn_angle, key_gain):
    turned_keys = ready_to_store(fresh_keys, turn_angle, key_gain)
    key_scale = lax.optimization_barrier(jnp.max(jnp.abs(turned_keys), axis=1))
    narrow_keys = (turned_keys / key_scale[:, None]).astype(jnp.bfloat16)
    decode_keys = jnp.transpose(narrow_keys, (0, 2, 3, 1))
    decode_values = fresh_values
    return (decode_keys, decode_values, key_scale)
```

```python
import functools

import jax
import jax.numpy as jnp
from jax import lax
from jax.experimental import pallas as pl
from jax.experimental.pallas import tpu as pltpu
from jax.sharding import PartitionSpec as P

MESH = pl.DeviceIdType.MESH
LANES = 128


def partner(me, k, n):
    if n & (n - 1) == 0:
        return me ^ k
    return lax.rem(k - me + n, n)


def order(nc, nf):
    steps = [(i, j) for j in range(nf - 1, -1, -1) for i in range(nc)]
    return steps


def kernel(nc, nf, heads, spots, keys, values, angle, gain, keys_out, values_out, scale_out,
           moved, turned, angles, gains, pick, peak, send_sem, key_sem, value_sem, own_sem):
    n = nc * nf
    size = gain.shape[-1]
    half = size // 2
    c, f, g = (lax.axis_index(a) for a in ("coarse", "fine", "group"))
    me = c * nf + f

    def device(i, j):
        return (i, j, g)

    barrier = pltpu.get_barrier_semaphore()
    for k in range(1, n):
        other = lax.rem(me + k, n)
        pl.semaphore_signal(
            barrier, inc=1, device_id=device(other // nf, lax.rem(other, nf)), device_id_type=MESH
        )
    pl.semaphore_wait(barrier, n - 1)

    steps = order(nc, nf)
    sends = []
    for which, (source, target, sem) in enumerate(((keys, moved, key_sem), (values, values_out, value_sem))):
        for step, (i, j) in enumerate(steps):
            if (i, j) == (0, 0):
                continue
            tc, tf = (partner(c, i, nc), partner(f, j, nf))
            copy = pltpu.make_async_remote_copy(
                src_ref=source.at[tc * nf + tf],
                dst_ref=target.at[me],
                send_sem=send_sem.at[which, step],
                recv_sem=sem.at[me],
                device_id=device(tc, tf),
                device_id_type=MESH,
            )
            copy.start()
            sends.append(copy)
    own_keys = pltpu.make_async_copy(keys.at[me], moved.at[me], own_sem.at[0])
    own_values = pltpu.make_async_copy(values.at[me], values_out.at[me], own_sem.at[1])
    own_angles = pltpu.make_async_copy(angle, angles, own_sem.at[2])
    own_keys.start()
    own_angles.start()
    own_values.start()

    chunk = LANES * heads
    row = lax.broadcasted_iota(jnp.int32, (chunk, chunk), 0)
    column = lax.broadcasted_iota(jnp.int32, (chunk, chunk), 1)
    wanted = (column % LANES) * heads + column // LANES
    pick[...] = jnp.where(row == wanted, 1.0, 0.0).astype(jnp.bfloat16)
    gains[...] = jnp.transpose(jnp.broadcast_to(gain[...], (LANES, size)))
    peak[...] = jnp.zeros_like(peak)
    own_keys.wait()
    own_angles.wait()
    own_values.wait()

    def block(source):
        @pl.loop(0, spots // LANES)
        def _(part):
            rows = pl.ds(pl.multiple_of(part * chunk, chunk), chunk)
            spot = pl.ds(pl.multiple_of(source * spots + part * LANES, LANES), LANES)
            flat = lax.dot_general(
                moved[source, rows, :], pick[...], (((0,), (0,)), ((), ())),
                preferred_element_type=jnp.float32,
            )
            turn = angles[:, spot]
            cosine, sine = (jnp.cos(turn), jnp.sin(turn))
            for h in range(heads):
                wide = flat[:, h * LANES:(h + 1) * LANES]
                power = jnp.sum(wide * wide, axis=0, keepdims=True) * (1.0 / size)
                wide = wide * lax.rsqrt(power + 1e-06) * gains[...]
                first, second = (wide[:half], wide[half:])
                low = first * cosine - second * sine
                high = second * cosine + first * sine
                turned[h, pl.ds(0, half), spot] = low
                turned[h, pl.ds(half, half), spot] = high
                peak[h, pl.ds(0, half), :] = jnp.maximum(peak[h, pl.ds(0, half), :], jnp.abs(low))
                peak[h, pl.ds(half, half), :] = jnp.maximum(peak[h, pl.ds(half, half), :], jnp.abs(high))

    block(me)

    def arrived(target, sem, source):
        return pltpu.make_async_copy(target.at[source], target.at[source], sem.at[source])

    @pl.loop(1, n)
    def _(k):
        step = n - k
        source = partner(c, lax.rem(step, nc), nc) * nf + partner(f, step // nc, nf)
        arrived(moved, key_sem, source).wait()
        block(source)

    for h in range(heads):
        scale_out[pl.ds(h, 1), :] = jnp.max(jnp.transpose(peak[h]), axis=0, keepdims=True)
        peak[h] = jnp.broadcast_to(1.0 / jnp.max(peak[h], axis=1, keepdims=True), (size, LANES))

    @pl.loop(0, n * spots // LANES)
    def _(part):
        spot = pl.ds(pl.multiple_of(part * LANES, LANES), LANES)
        for h in range(heads):
            keys_out[h, :, spot] = (turned[h, :, spot] * peak[h]).astype(jnp.bfloat16)

    @pl.loop(1, n)
    def _(k):
        source = lax.rem(me + k, n)
        arrived(values_out, value_sem, source).wait()

    for copy in sends:
        copy.wait_send()


def local(nc, nf, fresh_keys, fresh_values, turn_angle, key_gain):
    n, spots, heads, size = fresh_keys.shape
    length, half = turn_angle.shape
    rows = spots * heads
    anywhere = pl.BlockSpec(memory_space=pl.ANY)
    inside = pl.BlockSpec(memory_space=pltpu.VMEM)
    keys_out, values_out, scale_out = pl.pallas_call(
        functools.partial(kernel, nc, nf, heads, spots),
        out_shape=(
            pltpu.VMEM((heads, size, length), jnp.bfloat16),
            pltpu.VMEM((n, rows, size), jnp.bfloat16),
            jax.ShapeDtypeStruct((heads, size), jnp.float32),
        ),
        in_specs=[anywhere, anywhere, anywhere, inside],
        out_specs=[inside, inside, inside],
        scratch_shapes=[
            pltpu.VMEM((n, rows, size), jnp.bfloat16),
            pltpu.VMEM((heads, size, length), jnp.float32),
            pltpu.VMEM((half, length), jnp.float32),
            pltpu.VMEM((size, LANES), jnp.float32),
            pltpu.VMEM((LANES * heads, LANES * heads), jnp.bfloat16),
            pltpu.VMEM((heads, size, LANES), jnp.float32),
            pltpu.SemaphoreType.DMA((2, n)),
            pltpu.SemaphoreType.DMA((n,)),
            pltpu.SemaphoreType.DMA((n,)),
            pltpu.SemaphoreType.DMA((3,)),
        ],
        compiler_params=pltpu.CompilerParams(
            collective_id=0, has_side_effects=True, vmem_limit_bytes=36 * 2**20
        ),
    )(
        fresh_keys.reshape(n, rows, size),
        fresh_values.reshape(n, rows, size),
        jnp.transpose(turn_angle),
        key_gain.reshape(1, size),
    )
    return (
        keys_out.reshape(1, heads, size, length),
        values_out.reshape(1, length, heads, size),
        scale_out.reshape(1, heads, size),
    )


def solution(mesh):
    in_specs = (
        P(None, ("coarse", "fine"), "group", None),
        P(None, ("coarse", "fine"), "group", None),
        P(),
        P(),
    )
    out_specs = (
        P(("coarse", "fine"), "group", None, None),
        P(("coarse", "fine"), None, "group", None),
        P(("coarse", "fine"), "group", None),
    )
    run = functools.partial(local, mesh.shape["coarse"], mesh.shape["fine"])
    return jax.shard_map(run, mesh=mesh, in_specs=in_specs, out_specs=out_specs, check_vma=False)
```

```python
import functools

import jax
import jax.numpy as jnp
from jax import lax
from jax.experimental import pallas as pl
from jax.experimental.pallas import tpu as pltpu
from jax.sharding import PartitionSpec as P

MESH = pl.DeviceIdType.MESH
LANES = 128
PIECES = 4


def partner(me, k, n):
    if n & (n - 1) == 0:
        return me ^ k
    return lax.rem(k - me + n, n)


SPREAD = (
    (0, 3), (1, 0), (2, 0), (0, 2), (3, 0), (1, 3), (2, 1), (0, 1),
    (1, 2), (2, 3), (3, 1), (2, 2), (1, 1), (3, 3), (3, 2),
)


def plan(nc, nf):
    every = [(i, j) for i in range(nc) for j in range(nf - 1, -1, -1) if (i, j) != (0, 0)]
    steps = [step for step in SPREAD if step in every]
    steps += [step for step in every if step not in SPREAD]
    later = [steps[-1]] + steps[1:-1] + [steps[0]]
    return [(which, i, j) for which, some in enumerate((steps, later)) for i, j in some]


def kernel(nc, nf, heads, spots, keys, values, angle, gain, keys_out, values_out, scale_out,
           moved, turned, angles, gains, pick, peak, send_sem, key_sem, value_sem, own_sem):
    n = nc * nf
    size = gain.shape[-1]
    half = size // 2
    c, f, g = (lax.axis_index(a) for a in ("coarse", "fine", "group"))
    me = c * nf + f

    def device(i, j):
        return (i, j, g)

    barrier = pltpu.get_barrier_semaphore()
    for k in range(1, n):
        other = lax.rem(me + k, n)
        pl.semaphore_signal(
            barrier, inc=1, device_id=device(other // nf, lax.rem(other, nf)), device_id_type=MESH
        )
    pl.semaphore_wait(barrier, n - 1)

    sends = []
    for which, i, j in plan(nc, nf):
        source, target, sem = ((keys, moved, key_sem), (values, values_out, value_sem))[which]
        tc, tf = (partner(c, i, nc), partner(f, j, nf))
        copy = pltpu.make_async_remote_copy(
            src_ref=source.at[tc * nf + tf],
            dst_ref=target.at[me],
            send_sem=send_sem.at[which, i * nf + j],
            recv_sem=sem.at[me],
            device_id=device(tc, tf),
            device_id_type=MESH,
        )
        copy.start()
        sends.append(copy)
    own_keys = pltpu.make_async_copy(keys.at[me], moved.at[me], own_sem.at[0])
    own_values = pltpu.make_async_copy(values.at[me], values_out.at[me], own_sem.at[1])
    own_angles = pltpu.make_async_copy(angle, angles, own_sem.at[2])
    own_keys.start()
    own_angles.start()
    own_values.start()

    chunk = LANES * heads
    row = lax.broadcasted_iota(jnp.int32, (chunk, chunk), 0)
    column = lax.broadcasted_iota(jnp.int32, (chunk, chunk), 1)
    wanted = (column % LANES) * heads + column // LANES
    pick[...] = jnp.where(row == wanted, 1.0, 0.0).astype(jnp.bfloat16)
    gains[...] = jnp.transpose(jnp.broadcast_to(gain[...], (LANES, size)))
    peak[...] = jnp.zeros_like(peak)
    own_keys.wait()
    own_angles.wait()
    own_values.wait()

    def block(source):
        @pl.loop(0, spots // LANES)
        def _(part):
            rows = pl.ds(pl.multiple_of(part * chunk, chunk), chunk)
            spot = pl.ds(pl.multiple_of(source * spots + part * LANES, LANES), LANES)
            flat = lax.dot_general(
                moved[source, rows, :], pick[...], (((0,), (0,)), ((), ())),
                preferred_element_type=jnp.float32,
            )
            turn = angles[:, spot]
            cosine, sine = (jnp.cos(turn), jnp.sin(turn))
            for h in range(heads):
                wide = flat[:, h * LANES:(h + 1) * LANES]
                power = jnp.sum(wide * wide, axis=0, keepdims=True) * (1.0 / size)
                wide = wide * lax.rsqrt(power + 1e-06) * gains[...]
                first, second = (wide[:half], wide[half:])
                low = first * cosine - second * sine
                high = second * cosine + first * sine
                turned[h, pl.ds(0, half), spot] = low
                turned[h, pl.ds(half, half), spot] = high
                peak[h, pl.ds(0, half), :] = jnp.maximum(peak[h, pl.ds(0, half), :], jnp.abs(low))
                peak[h, pl.ds(half, half), :] = jnp.maximum(peak[h, pl.ds(half, half), :], jnp.abs(high))

    block(me)

    def arrived(target, sem, source):
        return pltpu.make_async_copy(target.at[source], target.at[source], sem.at[source])

    @pl.loop(1, n)
    def _(k):
        step = n - k
        source = partner(c, lax.rem(step, nc), nc) * nf + partner(f, step // nc, nf)
        arrived(moved, key_sem, source).wait()
        block(source)

    for h in range(heads):
        scale_out[pl.ds(h, 1), :] = jnp.max(jnp.transpose(peak[h]), axis=0, keepdims=True)
        peak[h] = jnp.broadcast_to(1.0 / jnp.max(peak[h], axis=1, keepdims=True), (size, LANES))

    @pl.loop(0, n * spots // LANES)
    def _(part):
        spot = pl.ds(pl.multiple_of(part * LANES, LANES), LANES)
        for h in range(heads):
            keys_out[h, :, spot] = (turned[h, :, spot] * peak[h]).astype(jnp.bfloat16)

    @pl.loop(1, n)
    def _(k):
        source = lax.rem(me + k, n)
        arrived(values_out, value_sem, source).wait()

    for copy in sends:
        copy.wait_send()


def leave(keys, values, scale, keys_out, values_out, scale_out, sem):
    pairs = [(scale, scale_out)]
    for source, target in ((values, values_out), (keys, keys_out)):
        cut = source.shape[0] // PIECES or 1
        pairs += [
            (source.at[pl.ds(at, cut)], target.at[pl.ds(at, cut)]) for at in range(0, source.shape[0], cut)
        ]
    copies = [pltpu.make_async_copy(a, b, sem.at[at]) for at, (a, b) in enumerate(pairs)]
    for copy in copies:
        copy.start()
    for copy in copies:
        copy.wait()


def local(nc, nf, fresh_keys, fresh_values, turn_angle, key_gain):
    n, spots, heads, size = fresh_keys.shape
    length, half = turn_angle.shape
    rows = spots * heads
    anywhere = pl.BlockSpec(memory_space=pl.ANY)
    inside = pl.BlockSpec(memory_space=pltpu.VMEM)
    keys_out, values_out, scale_out = pl.pallas_call(
        functools.partial(kernel, nc, nf, heads, spots),
        out_shape=(
            pltpu.VMEM((heads, size, length), jnp.bfloat16),
            pltpu.VMEM((n, rows, size), jnp.bfloat16),
            pltpu.VMEM((heads, size), jnp.float32),
        ),
        in_specs=[anywhere, anywhere, anywhere, inside],
        out_specs=[inside, inside, inside],
        scratch_shapes=[
            pltpu.VMEM((n, rows, size), jnp.bfloat16),
            pltpu.VMEM((heads, size, length), jnp.float32),
            pltpu.VMEM((half, length), jnp.float32),
            pltpu.VMEM((size, LANES), jnp.float32),
            pltpu.VMEM((LANES * heads, LANES * heads), jnp.bfloat16),
            pltpu.VMEM((heads, size, LANES), jnp.float32),
            pltpu.SemaphoreType.DMA((2, n)),
            pltpu.SemaphoreType.DMA((n,)),
            pltpu.SemaphoreType.DMA((n,)),
            pltpu.SemaphoreType.DMA((3,)),
        ],
        compiler_params=pltpu.CompilerParams(
            collective_id=0, has_side_effects=True, vmem_limit_bytes=36 * 2**20
        ),
    )(
        fresh_keys.reshape(n, rows, size),
        fresh_values.reshape(n, rows, size),
        jnp.transpose(turn_angle),
        key_gain.reshape(1, size),
    )
    keys_out, values_out, scale_out = pl.pallas_call(
        leave,
        out_shape=tuple(
            jax.ShapeDtypeStruct(a.shape, a.dtype) for a in (keys_out, values_out, scale_out)
        ),
        in_specs=[inside, inside, inside],
        out_specs=[anywhere, anywhere, anywhere],
        scratch_shapes=[pltpu.SemaphoreType.DMA((2 * n + 1,))],
        compiler_params=pltpu.CompilerParams(vmem_limit_bytes=2**20),
    )(keys_out, values_out, scale_out)
    return (
        keys_out.reshape(1, heads, size, length),
        values_out.reshape(1, length, heads, size),
        scale_out.reshape(1, heads, size),
    )


def solution(mesh):
    in_specs = (
        P(None, ("coarse", "fine"), "group", None),
        P(None, ("coarse", "fine"), "group", None),
        P(),
        P(),
    )
    out_specs = (
        P(("coarse", "fine"), "group", None, None),
        P(("coarse", "fine"), None, "group", None),
        P(("coarse", "fine"), "group", None),
    )
    run = functools.partial(local, mesh.shape["coarse"], mesh.shape["fine"])
    return jax.shard_map(run, mesh=mesh, in_specs=in_specs, out_specs=out_specs, check_vma=False)
```
